32 devices in a mesh: sub: 4 (over x, core), gx: 4 (over z), gy: 2 (over y).
Axes of the slice: x: 2, y: 2, z: 4, core: 2. Of those that a mesh axis runs over, the one named last changes fastest.
Arguments:
- state: float32 [4, 256, 512], P(None, ('sub', 'gx'), 'gy'), may hold values from -4 to 4
- damping: float32 [4, 256, 512], P(None, ('sub', 'gx'), 'gy'), may hold values from 0.005 to 0.1
- weights: float32 [4], replicated, may hold values from 0.5 to 1.5
Outputs:
- combined: float32 [4, 256, 512], P(None, ('sub', 'gx'), 'gy')
- column_error: float32 [4, 512], P(None, 'gy')
The draws below stay inside these ranges and needn't reach their ends.
All inputs are finite; a program needn't handle non-finite values.
Results may differ from the reference program's by a relative error of at most 0.0003.
Values sent between devices are 32-bit elements; how exact they have to be, the bound alone decides.
A program may use at most 64 MiB of HBM per device.

```python
import math
import jax
import jax.numpy as jnp
from jax import lax

FIELDS = 4
KRYLOV = 12
SUBSTEPS = 4
NX = 256
NY = 512


def block_scale(stream_key, dims, shards, smallest, top_value):
    factor_of = 1.0
    for dim, parts in shards:
        draws = jax.random.uniform(jax.random.fold_in(jax.random.fold_in(stream_key, 6), dim), (parts,), jnp.float32, smallest / len(shards), top_value / len(shards))
        factor_of = factor_of * jnp.repeat(jnp.exp(draws), dims[dim] // parts).reshape((-1,) + (1,) * (len(dims) - 1 - dim))
    return factor_of


def scatter_about(stream_key, shape, width, limit, pieces=(), kind=jnp.bfloat16):
    entries = jax.random.normal(stream_key, shape, jnp.float32) * width
    if len(pieces) > 0:
        entries = block_scale(stream_key, shape, pieces, -0.22, 0.18) * entries
    return jnp.clip(entries, min=-limit, max=limit).astype(kind)


def setup_inputs(seed: int = 0) -> dict:
    key_list = jax.random.split(jax.random.key(seed), 4)
    return {
        "state": scatter_about(key_list[0], (FIELDS, NX, NY), 1.0, 4.0, ((1, 16), (2, 2)), jnp.float32),
        "damping": jnp.clip(jnp.exp(math.log(0.1) - 2.9957323 * jax.random.uniform(key_list[1], (FIELDS, NX, NY), jnp.float32) ** block_scale(key_list[1], (FIELDS, NX, NY), ((1, 16), (2, 2)), -0.2, 0.2)), 0.005, 0.1),
        "weights": jnp.clip(jax.random.uniform(key_list[2], (SUBSTEPS,), jnp.float32, 0.5, 1.5), 0.5, 1.5),
    }


dt_total = 4.0
sound_sq = 1.0
buoyancy_sq = 0.5
norm_eps = 1e-06
taylor_degree = 12
squarings = 8

def tendencies(padded):
    velocity_x = padded[0]
    velocity_y = padded[1]
    buoyancy = padded[2]
    pressure = padded[3]
    rise_x = 0.5 * (pressure[2:, 1:-1] - pressure[:-2, 1:-1])
    rise_y = 0.5 * (pressure[1:-1, 2:] - pressure[1:-1, :-2])
    spread = 0.5 * (velocity_x[2:, 1:-1] - velocity_x[:-2, 1:-1]) + 0.5 * (velocity_y[1:-1, 2:] - velocity_y[1:-1, :-2])
    return jnp.stack([-rise_x, -rise_y + buoyancy[1:-1, 1:-1], -buoyancy_sq * velocity_y[1:-1, 1:-1], -sound_sq * spread])

def wave(field):
    return tendencies(jnp.pad(field, ((0, 0), (1, 1), (1, 1))))

def phi_first(hessenberg):
    extent = hessenberg.shape[0]
    augmented = jnp.zeros((extent + 1, extent + 1), jnp.float32)
    augmented = augmented.at[:extent, :extent].set(hessenberg).at[0, extent].set(1.0)
    scaled = augmented / 2.0 ** squarings
    result = jnp.eye(extent + 1, dtype=jnp.float32)
    power_term = result
    for degree in range(1, taylor_degree + 1):
        power_term = jnp.dot(power_term, scaled, precision=lax.Precision.HIGHEST) / degree
        result = result + power_term
    for repeat in range(squarings):
        result = jnp.dot(result, result, precision=lax.Precision.HIGHEST)
    return result[:extent, extent]

def reference(state, damping, weights):
    stiffness = 3.0 * damping * state * state
    forcing = wave(state) - damping * state * state * state
    beta_norm = jnp.sqrt(jnp.sum(forcing * forcing) + norm_eps)
    vectors = [forcing / beta_norm]
    hessenberg = jnp.zeros((KRYLOV + 1, KRYLOV), jnp.float32)
    for column in range(KRYLOV):
        current = vectors[column]
        image = dt_total * (wave(current) - stiffness * current)
        products = jnp.stack([jnp.sum(vector * image) for vector in vectors])
        for index_row in range(column + 1):
            image = image - products[index_row] * vectors[index_row]
        length = jnp.sqrt(jnp.sum(image * image) + norm_eps)
        hessenberg = hessenberg.at[:column + 1, column].set(products).at[column + 1, column].set(length)
        vectors.append(image / length)
    mixing = jnp.zeros((KRYLOV,), jnp.float32)
    highest = jnp.zeros((), jnp.float32)
    for member in range(SUBSTEPS):
        fraction = (member + 1) / SUBSTEPS
        factor = dt_total * fraction
        coefficients = phi_first(fraction * hessenberg[:KRYLOV])
        mixing = mixing + weights[member] * factor * beta_norm * coefficients
        estimate = factor * beta_norm * fraction * hessenberg[KRYLOV, KRYLOV - 1] * jnp.abs(coefficients[KRYLOV - 1])
        highest = jnp.maximum(highest, estimate)
    combined = state
    for index_row in range(KRYLOV):
        combined = combined + mixing[index_row] * vectors[index_row]
    column_error = highest * lax.optimization_barrier(jnp.max(jnp.abs(vectors[KRYLOV]), axis=1))
    return (combined, column_error)
```

```python
import functools

import jax
import jax.numpy as jnp
from jax import lax
from jax.experimental import pallas as pl
from jax.experimental.pallas import tpu as pltpu
from jax.sharding import PartitionSpec as P

KRYLOV = 12
SUBSTEPS = 4
BLOCK = 4

dt_total = 4.0
sound_sq = 1.0
buoyancy_sq = 0.5
norm_eps = 1e-06
squarings = 4

SIDE = 16
LANES = 128
MESH = pl.DeviceIdType.MESH
HIGH = lax.Precision.HIGHEST


def rise(cells, axis):
    extent = cells.shape[axis]
    return 0.5 * (pltpu.roll(cells, extent - 1, axis) - pltpu.roll(cells, 1, axis))


def wave(vx, vy, b, p):
    return (
        -rise(p, 0),
        -rise(p, 1) + b,
        -buoyancy_sq * vy,
        -sound_sq * (rise(vx, 0) + rise(vy, 1)),
    )


def dot(a, b):
    return jnp.dot(a, b, precision=HIGH, preferred_element_type=jnp.float32)


def kernel(sizes, state, damping, weights, combined, column_error,
           ext, basis, stiff, rows_ref, send, gather, peak_send, peak_gather,
           halo_send, halo_recv, red_send, red_recv, peak_sems):
    n_sub, n_gx, n_gy = sizes
    total = n_sub * n_gx * n_gy
    n_row = n_sub * n_gx
    fields, nx, ny = state.shape
    sub, gx, gy = lax.axis_index("sub"), lax.axis_index("gx"), lax.axis_index("gy")
    row = sub * n_gx + gx
    me = row * n_gy + gy

    def coords(flat):
        line = flat // n_gy
        return (line // n_gx, line % n_gx, flat % n_gy)

    barrier = pltpu.get_barrier_semaphore()

    @pl.loop(1, total)
    def _(d):
        pl.semaphore_signal(barrier, inc=1, device_id=coords((me + d) % total), device_id_type=MESH)

    ext[0, :, 0:nx, 0:ny] = state[...]
    ext[1, :, 0:nx, 0:ny] = damping[...]
    rows_ref[...] = jnp.zeros_like(rows_ref)
    pl.semaphore_wait(barrier, total - 1)

    dirs = [(dr, dc) for dr in (-1, 0, 1) for dc in (-1, 0, 1) if (dr, dc) != (0, 0)]

    def valid(dr, dc):
        r, c = row + dr, gy + dc
        return (r >= 0) & (r < n_row) & (c >= 0) & (c < n_gy)

    def halo_copy(k, a):
        dr, dc = dirs[k]
        r = row + dr
        dev = (r // n_gx, r % n_gx, gy + dc)
        lo = 0 if dc < 0 else ny - LANES
        source = (state, damping)[a]
        src = source if dc == 0 else source.at[:, :, lo : lo + LANES]
        return pltpu.make_async_remote_copy(
            src_ref=src, dst_ref=ext.at[region(a, -dr, -dc)],
            send_sem=halo_send.at[2 * k + a], recv_sem=halo_recv.at[2 * k + a],
            device_id=dev, device_id_type=MESH)

    def region(a, dr, dc):
        r0 = {0: 0, 1: nx, -1: 2 * nx}[dr]
        c0, c1 = {0: (0, ny), 1: (ny, ny + LANES), -1: (ny + LANES, ny + 2 * LANES)}[dc]
        return (a, slice(None), slice(r0, r0 + nx), slice(c0, c1))

    for k, (dr, dc) in enumerate(dirs):
        @pl.when(valid(dr, dc))
        def _(k=k):
            for a in range(2):
                halo_copy(k, a).start()

        @pl.when(jnp.logical_not(valid(dr, dc)))
        def _(dr=dr, dc=dc):
            for a in range(2):
                where = region(a, dr, dc)
                ext[where] = jnp.zeros(ext[where].shape, jnp.float32)

    for k, (dr, dc) in enumerate(dirs):
        @pl.when(valid(-dr, -dc))
        def _(k=k):
            for a in range(2):
                halo_copy(k, a).wait_recv()

        @pl.when(valid(dr, dc))
        def _(k=k):
            for a in range(2):
                halo_copy(k, a).wait_send()

    height, width = 3 * nx, ny + LANES
    lane = lax.broadcasted_iota(jnp.int32, (height, LANES), 1)
    half = lane < LANES // 2

    def extended(a, f):
        side = jnp.where(half, ext[a, f, :, ny : ny + LANES], ext[a, f, :, ny + LANES : ny + 2 * LANES])
        return jnp.concatenate([ext[a, f, :, 0:ny], side], axis=1)

    rr = lax.broadcasted_iota(jnp.int32, (height, width), 0)
    cc = lax.broadcasted_iota(jnp.int32, (height, width), 1)
    has_next, has_prev = (row < n_row - 1).astype(jnp.int32), (row > 0).astype(jnp.int32)
    has_right, has_left = (gy < n_gy - 1).astype(jnp.int32), (gy > 0).astype(jnp.int32)
    row_in = jnp.where(rr < nx, 1, jnp.where(rr < 2 * nx, has_next, has_prev))
    col_in = jnp.where(cc < ny, 1, jnp.where(cc < ny + LANES // 2, has_right, has_left))
    mask = (row_in * col_in).astype(jnp.float32)

    start = [extended(0, f) for f in range(fields)]
    waves = wave(*start)
    for f in range(fields):
        damp = extended(1, f)
        s = start[f]
        stiff[f] = 3.0 * damp * s * s
        basis[0, f] = mask * (waves[f] - damp * s * s * s)

    ri = lax.broadcasted_iota(jnp.int32, (SIDE, SIDE), 0)
    ci = lax.broadcasted_iota(jnp.int32, (SIDE, SIDE), 1)
    eye = ri == ci
    li = lax.broadcasted_iota(jnp.int32, (1, SIDE), 1)

    def to_column(r):
        return jnp.sum(jnp.where(eye, r, 0.0), axis=1, keepdims=True)

    def to_row(c):
        return jnp.sum(jnp.where(eye, c, 0.0), axis=0, keepdims=True)

    def single(x):
        return jnp.sum(jnp.sum(x, axis=1, keepdims=True), axis=0, keepdims=True)

    def combine(columns):
        return jnp.sum(columns, axis=0, keepdims=True)

    gram = jnp.zeros((SIDE, SIDE), jnp.float32)
    hess = jnp.zeros((SIDE, SIDE), jnp.float32)
    beta = None
    syncs = KRYLOV // BLOCK
    for s in range(syncs):
        base = s * BLOCK
        count = base + BLOCK + 1
        if s == 0:
            shift = jnp.full((1, 1), 3.0, jnp.float32)
            back = jnp.full((1, 1), 4.0, jnp.float32)
            grow = jnp.full((1, 1), 5.0, jnp.float32)
        else:
            recent = (ri >= base - 3) & (ri < base)
            third = 1.0 / 3.0
            shift = -third * single(jnp.where(recent & eye, hess, 0.0))
            back = -third * single(jnp.where(recent & (ci == ri - 1), hess, 0.0))
            grow = third * single(jnp.where(recent & (ci == ri + 1), hess, 0.0))
        inverse = 1.0 / grow
        for j in range(BLOCK):
            at = base + j
            current = [basis[at, f] for f in range(fields)]
            waves = wave(*current)
            for f in range(fields):
                image = dt_total * (mask * waves[f] - stiff[f] * current[f]) + shift * current[f]
                if j > 0:
                    image = image + back * basis[at - 1, f]
                basis[at + 1, f] = image * inverse

        first = 0 if s <= 1 else base - BLOCK + 1
        offset, offsets = 0, {}
        for j in range(first, count):
            offsets[j] = offset
            left = basis[j, :, 0:nx, 0:ny]
            for i in range(j + 1):
                prod = left * basis[i, :, 0:nx, 0:ny]
                prod = jnp.sum(prod, axis=0)
                prod = prod.reshape(nx // 8, 8, ny).sum(axis=0)
                acc = prod[:, 0:LANES]
                for t in range(LANES, ny, LANES):
                    acc = acc + prod[:, t : t + LANES]
                rows_ref[offset + i : offset + i + 1, :] = jnp.sum(acc, axis=0, keepdims=True)
            offset += j + 1
        packed = lax.dot_general(
            jnp.ones((8, LANES), jnp.float32), rows_ref[...], (((1,), (1,)), ((), ())),
            precision=HIGH, preferred_element_type=jnp.float32)[0:1, :]
        send[s] = packed
        gather[s, me] = packed

        @pl.loop(1, total)
        def _(d, s=s):
            pltpu.make_async_remote_copy(
                src_ref=send.at[s], dst_ref=gather.at[s, me],
                send_sem=red_send.at[s], recv_sem=red_recv.at[s],
                device_id=coords((me + d) % total), device_id_type=MESH).start()

        everyone = pltpu.make_async_remote_copy(
            src_ref=gather.at[s, pl.ds(0, total - 1)], dst_ref=gather.at[s, pl.ds(0, total - 1)],
            send_sem=red_send.at[s], recv_sem=red_recv.at[s],
            device_id=coords((me + 1) % total), device_id_type=MESH)
        everyone.wait_recv()
        everyone.wait_send()
        summed = jnp.sum(gather[s], axis=0)

        fresh = jnp.zeros((SIDE, LANES), jnp.float32)
        fr = lax.broadcasted_iota(jnp.int32, (SIDE, LANES), 0)
        fl = lax.broadcasted_iota(jnp.int32, (SIDE, LANES), 1)
        for j in range(first, count):
            line = summed if offsets[j] == 0 else pltpu.roll(summed, LANES - offsets[j], 1)
            fresh = jnp.where((fr == j) & (fl <= j), line, fresh)
        lower = fresh[:, 0:SIDE]
        upper = fresh.T[0:SIDE, :]
        old = (ri < first) & (ci < first)
        gram = jnp.where(old, gram, jnp.where(ci <= ri, lower, upper))

        bt = jnp.where(ri < base, hess, 0.0)
        cand = (ri >= base) & (ri < base + BLOCK)
        bt = bt + jnp.where(cand & (ci == ri + 1), grow, 0.0) - jnp.where(cand & eye, shift, 0.0)
        bt = bt - jnp.where(cand & (ri > base) & (ci == ri - 1), back, 0.0)
        btg = dot(bt, gram)

        if s == 0:
            beta = jnp.sqrt(gram[0:1, 0:1] + norm_eps)
            known = ri < 1
            rt = jnp.where(known & eye, 1.0, 0.0) / beta
            grt = jnp.where(known, gram, 0.0) / beta
            r_col = jnp.where(ri[:, 0:1] == 0, 1.0 / beta, 0.0)
        else:
            known = ri <= base
            rt = jnp.where(known & eye, 1.0, 0.0)
            grt = jnp.where(known, gram, 0.0)
            r_col = jnp.where(ri[:, 0:1] == base, 1.0, 0.0)
        for q in range(base, base + BLOCK):
            w = combine(bt * r_col)
            u = combine(btg * r_col)
            h = jnp.sum(rt * u, axis=1, keepdims=True)
            z = w - combine(rt * h)
            gz = u - combine(grt * h)
            squared = jnp.sum(z * gz, axis=1, keepdims=True)
            z_col = to_column(z)
            length = jnp.sqrt(jnp.maximum(squared, 0.0) + norm_eps)
            scale = 1.0 / length
            r_col = z_col * scale
            rt = jnp.where(ri == q + 1, z * scale, rt)
            grt = jnp.where(ri == q + 1, gz * scale, grt)
            hess = jnp.where(ri == q, to_row(h) + jnp.where(li == q + 1, length, 0.0), hess)

        if s < syncs - 1:
            targets = range(0 if s == 0 else base + 1, count)
            coefs = {q: [rt[q : q + 1, j : j + 1] for j in range(count)] for q in targets}

            @pl.loop(0, fields * (height // 8))
            def _(t, targets=targets, coefs=coefs, count=count):
                f, r = t // (height // 8), pl.multiple_of((t % (height // 8)) * 8, 8)
                sums = {q: None for q in targets}
                for j in range(count):
                    vec = basis[j, f, pl.ds(r, 8), :]
                    for q in targets:
                        if j <= q:
                            term = coefs[q][j] * vec
                            sums[q] = term if sums[q] is None else sums[q] + term
                for q in targets:
                    basis[q, f, pl.ds(r, 8), :] = sums[q]

    tail = KRYLOV

    def owned(coef_row):
        out = None
        for j in range(KRYLOV + 1):
            term = coef_row[0:1, j : j + 1].reshape(1, 1, 1) * basis[j, :, 0:nx, 0:ny]
            out = term if out is None else out + term
        return out

    last = owned(rt[tail : tail + 1, :])
    peak = jnp.max(jnp.abs(last), axis=1)
    peak_send[...] = peak
    peak_gather[row] = peak

    @pl.loop(1, n_row)
    def _(d):
        to = (row + d) % n_row
        pltpu.make_async_remote_copy(
            src_ref=peak_send, dst_ref=peak_gather.at[row],
            send_sem=peak_sems.at[0], recv_sem=peak_sems.at[1],
            device_id=(to // n_gx, to % n_gx, gy), device_id_type=MESH).start()

    inside = (ri < KRYLOV) & (ci < KRYLOV)
    x = jnp.where(inside, hess / SUBSTEPS, 0.0) + jnp.where((ri == KRYLOV) & (ci == 0), 1.0, 0.0)
    x = x / 2.0**squarings
    ident = jnp.where(eye, 1.0, 0.0)
    x2 = dot(x, x)
    x3 = dot(x2, x)
    x4 = dot(x2, x2)
    fact = [1.0]
    for d in range(1, 13):
        fact.append(fact[-1] / d)

    def poly(d):
        return fact[d] * ident + fact[d + 1] * x + fact[d + 2] * x2 + fact[d + 3] * x3

    power = poly(0) + dot(x4, poly(4) + dot(x4, poly(8) + fact[12] * x4))
    for repeat in range(squarings):
        power = dot(power, power)
    powers = [None, power]
    for member in range(2, SUBSTEPS + 1):
        powers.append(dot(powers[member // 2], powers[member - member // 2]))
    mixing = jnp.zeros((1, SIDE), jnp.float32)
    highest = jnp.zeros((1, 1), jnp.float32)
    tip = hess[KRYLOV - 1 : KRYLOV, KRYLOV : KRYLOV + 1]
    for member in range(SUBSTEPS):
        line = powers[member + 1][KRYLOV : KRYLOV + 1, :]
        part = (dt_total / SUBSTEPS) * beta * line
        mixing = mixing + weights[member] * part
        fraction = (member + 1) / SUBSTEPS
        highest = jnp.maximum(highest, fraction * tip * jnp.abs(part[:, KRYLOV - 1 : KRYLOV]))
    mixing = jnp.where(li < KRYLOV, mixing, 0.0)
    combined[...] = state[...] + owned(combine(rt * to_column(mixing)))

    around = pltpu.make_async_remote_copy(
        src_ref=peak_gather.at[pl.ds(0, n_row - 1)], dst_ref=peak_gather.at[pl.ds(0, n_row - 1)],
        send_sem=peak_sems.at[0], recv_sem=peak_sems.at[1],
        device_id=coords((me + n_gy) % total), device_id_type=MESH)
    around.wait_recv()
    around.wait_send()
    column_error[...] = highest * jnp.max(peak_gather[...], axis=0)


def shards(sizes, state, damping, weights):
    fields, nx, ny = state.shape
    n_sub, n_gx, n_gy = sizes
    total = n_sub * n_gx * n_gy
    syncs = KRYLOV // BLOCK
    vmem = pl.BlockSpec(memory_space=pltpu.VMEM)
    return pl.pallas_call(
        functools.partial(kernel, sizes),
        out_shape=(
            jax.ShapeDtypeStruct(state.shape, jnp.float32),
            jax.ShapeDtypeStruct((fields, ny), jnp.float32),
        ),
        in_specs=[vmem, vmem, pl.BlockSpec(memory_space=pltpu.SMEM)],
        out_specs=(vmem, vmem),
        scratch_shapes=[
            pltpu.VMEM((2, fields, 3 * nx, ny + 2 * LANES), jnp.float32),
            pltpu.VMEM((KRYLOV + 1, fields, 3 * nx, ny + LANES), jnp.float32),
            pltpu.VMEM((fields, 3 * nx, ny + LANES), jnp.float32),
            pltpu.VMEM((LANES, LANES), jnp.float32),
            pltpu.VMEM((syncs, 1, LANES), jnp.float32),
            pltpu.VMEM((syncs, total, 1, LANES), jnp.float32),
            pltpu.VMEM((fields, ny), jnp.float32),
            pltpu.VMEM((n_sub * n_gx, fields, ny), jnp.float32),
            pltpu.SemaphoreType.DMA((16,)),
            pltpu.SemaphoreType.DMA((16,)),
            pltpu.SemaphoreType.DMA((syncs,)),
            pltpu.SemaphoreType.DMA((syncs,)),
            pltpu.SemaphoreType.DMA((2,)),
        ],
        compiler_params=pltpu.CompilerParams(
            collective_id=0, has_side_effects=True, vmem_limit_bytes=48 * 2**20),
    )(state, damping, weights)


def solution(mesh):
    sizes = (mesh.shape["sub"], mesh.shape["gx"], mesh.shape["gy"])
    return jax.shard_map(
        functools.partial(shards, sizes),
        mesh=mesh,
        in_specs=(P(None, ("sub", "gx"), "gy"), P(None, ("sub", "gx"), "gy"), P()),
        out_specs=(P(None, ("sub", "gx"), "gy"), P(None, "gy")),
        check_vma=False,
    )
```

```python
import functools

import jax
import jax.numpy as jnp
from jax import lax
from jax.experimental import pallas as pl
from jax.experimental.pallas import tpu as pltpu
from jax.sharding import PartitionSpec as P

KRYLOV = 12
SUBSTEPS = 4
BLOCK = 4

dt_total = 4.0
sound_sq = 1.0
buoyancy_sq = 0.5
norm_eps = 1e-06
squarings = 4

SIDE = 16
LANES = 128
MESH = pl.DeviceIdType.MESH
HIGH = lax.Precision.HIGHEST


def rise(cells, axis):
    extent = cells.shape[axis]
    return 0.5 * (pltpu.roll(cells, extent - 1, axis) - pltpu.roll(cells, 1, axis))


def wave(vx, vy, b, p):
    return (
        -rise(p, 0),
        -rise(p, 1) + b,
        -buoyancy_sq * vy,
        -sound_sq * (rise(vx, 0) + rise(vy, 1)),
    )


def dot(a, b):
    return jnp.dot(a, b, precision=HIGH, preferred_element_type=jnp.float32)


def kernel(sizes, state, damping, weights, combined, column_error,
           ext, edge_send, edge_recv, basis, begin, stiff, rows_ref, send, gather,
           peak_send, peak_gather, load_sems, halo_send, halo_recv, red_send, red_recv, peak_sems):
    n_sub, n_gx, n_gy = sizes
    total = n_sub * n_gx * n_gy
    n_row = n_sub * n_gx
    fields, nx, ny = state.shape
    sub, gx, gy = lax.axis_index("sub"), lax.axis_index("gx"), lax.axis_index("gy")
    row = sub * n_gx + gx
    me = row * n_gy + gy

    def coords(flat):
        line = flat // n_gy
        return (line // n_gx, line % n_gx, flat % n_gy)

    barrier = pltpu.get_barrier_semaphore()
    loads = [
        pltpu.make_async_copy(src, ext.at[a, :, 0:nx, :], load_sems.at[a])
        for a, src in enumerate((state, damping))
    ]
    for load in loads:
        load.start()

    subs = [lax.rem(sub + d, n_sub) for d in range(n_sub)]
    gxs = [lax.rem(gx + d, n_gx) for d in range(n_gx)]
    gys = [lax.rem(gy + d, n_gy) for d in range(n_gy)]

    def ring(d, extent):
        return min(d, extent - d)

    others = sorted(
        ((a, b, c) for a in range(n_sub) for b in range(n_gx) for c in range(n_gy)),
        key=lambda o: -(ring(o[1], n_gx) + ring(o[0], n_sub) + ring(o[2], n_gy)))[:-1]

    def each_other(visit):
        if total <= 64:
            for a, b, c in others:
                visit((subs[a], gxs[b], gys[c]))
        else:
            @pl.loop(1, total)
            def _(d):
                visit(coords((me + d) % total))

    each_other(lambda dev: pl.semaphore_signal(barrier, inc=1, device_id=dev, device_id_type=MESH))

    rows_ref[...] = jnp.zeros_like(rows_ref)
    begin[...] = jnp.zeros_like(begin)
    for load in loads:
        load.wait()

    edge = LANES // (2 * fields)
    tile_lane = lax.broadcasted_iota(jnp.int32, (nx, LANES), 1)
    for side in range(2):
        packed = jnp.zeros((nx, LANES), jnp.float32)
        for a in range(2):
            for f in range(fields):
                g = a * fields + f
                lo = 0 if side == 0 else ny - LANES
                turn = (edge * g + (0 if side == 0 else edge)) % LANES
                tile = ext[a, f, 0:nx, lo : lo + LANES]
                tile = tile if turn == 0 else pltpu.roll(tile, turn, 1)
                packed = jnp.where(tile_lane // edge == g, tile, packed)
        edge_send[side] = packed
    pl.semaphore_wait(barrier, total - 1)

    dirs = [(dr, dc) for dr in (-1, 1) for dc in (0, -1, 1)] + [(0, -1), (0, 1)]
    offset_of = {0: 0, 1: nx, -1: 2 * nx}

    def valid(dr, dc):
        r, c = row + dr, gy + dc
        return (r >= 0) & (r < n_row) & (c >= 0) & (c < n_gy)

    def landing(dr, dc):
        return edge_recv.at[dr + 1, (dc + 1) // 2]

    def halo_copies(k):
        dr, dc = dirs[k]
        r = row + dr
        dev = (r // n_gx, r % n_gx, gy + dc)
        if dc == 0:
            o = offset_of[-dr]
            pairs = [(ext.at[a, :, 0:nx, :], ext.at[a, :, o : o + nx, :]) for a in range(2)]
        else:
            pairs = [(edge_send.at[(dc + 1) // 2], landing(-dr, -dc))]
        return [
            pltpu.make_async_remote_copy(
                src_ref=src, dst_ref=dst,
                send_sem=halo_send.at[2 * k + n], recv_sem=halo_recv.at[2 * k + n],
                device_id=dev, device_id_type=MESH)
            for n, (src, dst) in enumerate(pairs)
        ]

    for k, (dr, dc) in enumerate(dirs):
        @pl.when(valid(dr, dc))
        def _(k=k):
            for copy in halo_copies(k):
                copy.start()

        @pl.when(jnp.logical_not(valid(dr, dc)))
        def _(dr=dr, dc=dc):
            if dc == 0:
                o = offset_of[dr]
                ext[:, :, o : o + nx, :] = jnp.zeros((2, fields, nx, ny), jnp.float32)
            else:
                edge_recv[dr + 1, (dc + 1) // 2] = jnp.zeros((nx, LANES), jnp.float32)

    for k, (dr, dc) in enumerate(dirs):
        @pl.when(valid(-dr, -dc))
        def _(k=k):
            for copy in halo_copies(k):
                copy.wait_recv()

        @pl.when(valid(dr, dc))
        def _(k=k):
            for copy in halo_copies(k):
                copy.wait_send()

    height, width = 3 * nx, ny + LANES
    lane = lax.broadcasted_iota(jnp.int32, (height, LANES), 1)
    sides = [
        jnp.concatenate([edge_recv[1, side], edge_recv[2, side], edge_recv[0, side]], axis=0)
        for side in range(2)
    ]

    def extended(a, f):
        g = a * fields + f

        def turned(cells, by):
            return cells if by % LANES == 0 else pltpu.roll(cells, by % LANES, 1)

        left = turned(sides[0], -edge * g - edge)
        right = turned(sides[1], -edge * g)
        side = jnp.where(lane < edge, right, jnp.where(lane >= LANES - edge, left, 0.0))
        return jnp.concatenate([ext[a, f], side], axis=1)

    rr = lax.broadcasted_iota(jnp.int32, (height, width), 0)
    cc = lax.broadcasted_iota(jnp.int32, (height, width), 1)
    has_next, has_prev = (row < n_row - 1).astype(jnp.int32), (row > 0).astype(jnp.int32)
    has_right, has_left = (gy < n_gy - 1).astype(jnp.int32), (gy > 0).astype(jnp.int32)
    row_in = jnp.where(rr < nx, 1, jnp.where(rr < 2 * nx, has_next, has_prev))
    col_in = jnp.where(cc < ny, 1, jnp.where(cc < ny + LANES // 2, has_right, has_left))
    mask = (row_in * col_in).astype(jnp.float32)

    start = [extended(0, f) for f in range(fields)]
    waves = wave(*start)
    for f in range(fields):
        damp = extended(1, f)
        s = start[f]
        stiff[f] = 3.0 * damp * s * s
        basis[0, f] = mask * (waves[f] - damp * s * s * s)

    ri = lax.broadcasted_iota(jnp.int32, (SIDE, SIDE), 0)
    ci = lax.broadcasted_iota(jnp.int32, (SIDE, SIDE), 1)
    eye = ri == ci
    li = lax.broadcasted_iota(jnp.int32, (1, SIDE), 1)

    def to_column(r):
        return jnp.sum(jnp.where(eye, r, 0.0), axis=1, keepdims=True)

    def to_row(c):
        return jnp.sum(jnp.where(eye, c, 0.0), axis=0, keepdims=True)

    def single(x):
        return jnp.sum(jnp.sum(x, axis=1, keepdims=True), axis=0, keepdims=True)

    def combine(columns):
        return jnp.sum(columns, axis=0, keepdims=True)

    raw_gram = jnp.zeros((SIDE, SIDE), jnp.float32)
    raw_rt = jnp.zeros((SIDE, SIDE), jnp.float32)
    hess = jnp.zeros((SIDE, SIDE), jnp.float32)
    beta = None
    syncs = KRYLOV // BLOCK
    for s in range(syncs):
        base = s * BLOCK
        count = base + BLOCK + 1
        if s == 0:
            shift = jnp.full((1, 1), 3.0, jnp.float32)
            back = jnp.full((1, 1), 4.0, jnp.float32)
            grow = jnp.full((1, 1), 5.0, jnp.float32)
        else:
            recent = (ri >= base - 3) & (ri < base)
            third = 1.0 / 3.0
            shift = -third * single(jnp.where(recent & eye, hess, 0.0))
            back = -third * single(jnp.where(recent & (ci == ri - 1), hess, 0.0))
            grow = third * single(jnp.where(recent & (ci == ri + 1), hess, 0.0))
        inverse = 1.0 / grow
        for j in range(BLOCK):
            at = base + j
            source = begin if j == 0 and s > 0 else basis.at[at]
            before = begin if j == 1 and s > 0 else basis.at[max(at - 1, 0)]
            current = [source[f] for f in range(fields)]
            waves = wave(*current)
            for f in range(fields):
                image = dt_total * (mask * waves[f] - stiff[f] * current[f]) + shift * current[f]
                if j > 0:
                    image = image + back * before[f]
                basis[at + 1, f] = image * inverse

        first = 0 if s == 0 else base + 1
        offset, offsets = 0, {}
        for j in range(first, count):
            offsets[j] = offset
            left = basis[j, :, 0:nx, 0:ny]
            for i in range(j + 1):
                prod = left * basis[i, :, 0:nx, 0:ny]
                prod = jnp.sum(prod, axis=0)
                prod = prod.reshape(nx // 8, 8, ny).sum(axis=0)
                acc = prod[:, 0:LANES]
                for t in range(LANES, ny, LANES):
                    acc = acc + prod[:, t : t + LANES]
                rows_ref[offset + i : offset + i + 1, :] = jnp.sum(acc, axis=0, keepdims=True)
            offset += j + 1
        packed = lax.dot_general(
            jnp.ones((8, LANES), jnp.float32), rows_ref[...], (((1,), (1,)), ((), ())),
            precision=HIGH, preferred_element_type=jnp.float32)[0:1, :]
        send[s] = packed
        gather[s, me] = packed

        each_other(lambda dev, s=s: pltpu.make_async_remote_copy(
            src_ref=send.at[s], dst_ref=gather.at[s, me],
            send_sem=red_send.at[s], recv_sem=red_recv.at[s],
            device_id=dev, device_id_type=MESH).start())

        everyone = pltpu.make_async_remote_copy(
            src_ref=gather.at[s, pl.ds(0, total - 1)], dst_ref=gather.at[s, pl.ds(0, total - 1)],
            send_sem=red_send.at[s], recv_sem=red_recv.at[s],
            device_id=coords((me + 1) % total), device_id_type=MESH)
        everyone.wait_recv()
        everyone.wait_send()
        summed = jnp.sum(gather[s], axis=0)

        fresh = jnp.zeros((SIDE, LANES), jnp.float32)
        fr = lax.broadcasted_iota(jnp.int32, (SIDE, LANES), 0)
        fl = lax.broadcasted_iota(jnp.int32, (SIDE, LANES), 1)
        for j in range(first, count):
            line = summed if offsets[j] == 0 else pltpu.roll(summed, LANES - offsets[j], 1)
            fresh = jnp.where((fr == j) & (fl <= j), line, fresh)
        lower = fresh[:, 0:SIDE]
        upper = fresh.T[0:SIDE, :]
        old = (ri < first) & (ci < first)
        raw_gram = jnp.where(old, raw_gram, jnp.where(ci <= ri, lower, upper))
        if s == 0:
            gram = raw_gram
        else:
            frame = jnp.where(ri <= base, raw_rt, jnp.where(eye, 1.0, 0.0))
            gram = lax.dot_general(
                dot(frame, raw_gram), frame, (((1,), (1,)), ((), ())),
                precision=HIGH, preferred_element_type=jnp.float32)

        bt = jnp.where(ri < base, hess, 0.0)
        cand = (ri >= base) & (ri < base + BLOCK)
        bt = bt + jnp.where(cand & (ci == ri + 1), grow, 0.0) - jnp.where(cand & eye, shift, 0.0)
        bt = bt - jnp.where(cand & (ri > base) & (ci == ri - 1), back, 0.0)
        btg = dot(bt, gram)

        if s == 0:
            beta = jnp.sqrt(gram[0:1, 0:1] + norm_eps)
            known = ri < 1
            rt = jnp.where(known & eye, 1.0, 0.0) / beta
            grt = jnp.where(known, gram, 0.0) / beta
            r_col = jnp.where(ri[:, 0:1] == 0, 1.0 / beta, 0.0)
        else:
            known = ri <= base
            rt = jnp.where(known & eye, 1.0, 0.0)
            grt = jnp.where(known, gram, 0.0)
            r_col = jnp.where(ri[:, 0:1] == base, 1.0, 0.0)
        for q in range(base, base + BLOCK):
            w = combine(bt * r_col)
            u = combine(btg * r_col)
            h = jnp.sum(rt * u, axis=1, keepdims=True)
            z = w - combine(rt * h)
            gz = u - combine(grt * h)
            squared = jnp.sum(z * gz, axis=1, keepdims=True)
            z_col = to_column(z)
            length = jnp.sqrt(jnp.maximum(squared, 0.0) + norm_eps)
            scale = 1.0 / length
            r_col = z_col * scale
            rt = jnp.where(ri == q + 1, z * scale, rt)
            grt = jnp.where(ri == q + 1, gz * scale, grt)
            hess = jnp.where(ri == q, to_row(h) + jnp.where(li == q + 1, length, 0.0), hess)

        raw_rt = rt if s == 0 else dot(rt, frame)
        if s < syncs - 1:
            top = count - 1
            coefs = [raw_rt[top : top + 1, j : j + 1] for j in range(count)]
            tiles = list(range((nx + 8) // 8)) + [height // 8 - 1]
            for f in range(fields):
                for t in tiles:
                    out = None
                    for j in range(count):
                        term = coefs[j] * basis[j, f, 8 * t : 8 * t + 8, :]
                        out = term if out is None else out + term
                    begin[f, 8 * t : 8 * t + 8, :] = out

    tail = KRYLOV

    def owned(coef_row):
        out = None
        for j in range(KRYLOV + 1):
            term = coef_row[0:1, j : j + 1].reshape(1, 1, 1) * basis[j, :, 0:nx, 0:ny]
            out = term if out is None else out + term
        return out

    last = owned(raw_rt[tail : tail + 1, :])
    peak = jnp.max(jnp.abs(last), axis=1)
    peak_send[...] = peak
    peak_gather[row] = peak

    @pl.loop(1, n_row)
    def _(d):
        to = (row + d) % n_row
        pltpu.make_async_remote_copy(
            src_ref=peak_send, dst_ref=peak_gather.at[row],
            send_sem=peak_sems.at[0], recv_sem=peak_sems.at[1],
            device_id=(to // n_gx, to % n_gx, gy), device_id_type=MESH).start()

    inside = (ri < KRYLOV) & (ci < KRYLOV)
    x = jnp.where(inside, hess / SUBSTEPS, 0.0) + jnp.where((ri == KRYLOV) & (ci == 0), 1.0, 0.0)
    x = x / 2.0**squarings
    ident = jnp.where(eye, 1.0, 0.0)
    x2 = dot(x, x)
    x3 = dot(x2, x)
    x4 = dot(x2, x2)
    fact = [1.0]
    for d in range(1, 13):
        fact.append(fact[-1] / d)

    def poly(d):
        return fact[d] * ident + fact[d + 1] * x + fact[d + 2] * x2 + fact[d + 3] * x3

    power = poly(0) + dot(x4, poly(4) + dot(x4, poly(8) + fact[12] * x4))
    for repeat in range(squarings):
        power = dot(power, power)
    powers = [None, power]
    for member in range(2, SUBSTEPS + 1):
        powers.append(dot(powers[member // 2], powers[member - member // 2]))
    mixing = jnp.zeros((1, SIDE), jnp.float32)
    highest = jnp.zeros((1, 1), jnp.float32)
    tip = hess[KRYLOV - 1 : KRYLOV, KRYLOV : KRYLOV + 1]
    for member in range(SUBSTEPS):
        line = powers[member + 1][KRYLOV : KRYLOV + 1, :]
        part = (dt_total / SUBSTEPS) * beta * line
        mixing = mixing + weights[member] * part
        fraction = (member + 1) / SUBSTEPS
        highest = jnp.maximum(highest, fraction * tip * jnp.abs(part[:, KRYLOV - 1 : KRYLOV]))
    mixing = jnp.where(li < KRYLOV, mixing, 0.0)
    combined[...] = ext[0, :, 0:nx, :] + owned(combine(raw_rt * to_column(mixing)))

    around = pltpu.make_async_remote_copy(
        src_ref=peak_gather.at[pl.ds(0, n_row - 1)], dst_ref=peak_gather.at[pl.ds(0, n_row - 1)],
        send_sem=peak_sems.at[0], recv_sem=peak_sems.at[1],
        device_id=coords((me + n_gy) % total), device_id_type=MESH)
    around.wait_recv()
    around.wait_send()
    column_error[...] = highest * jnp.max(peak_gather[...], axis=0)


def shards(sizes, state, damping, weights):
    fields, nx, ny = state.shape
    n_sub, n_gx, n_gy = sizes
    total = n_sub * n_gx * n_gy
    syncs = KRYLOV // BLOCK
    vmem = pl.BlockSpec(memory_space=pltpu.VMEM)
    return pl.pallas_call(
        functools.partial(kernel, sizes),
        out_shape=(
            jax.ShapeDtypeStruct(state.shape, jnp.float32),
            jax.ShapeDtypeStruct((fields, ny), jnp.float32),
        ),
        in_specs=[pl.BlockSpec(memory_space=pl.ANY)] * 2 + [pl.BlockSpec(memory_space=pltpu.SMEM)],
        out_specs=(vmem, vmem),
        scratch_shapes=[
            pltpu.VMEM((2, fields, 3 * nx, ny), jnp.float32),
            pltpu.VMEM((2, nx, LANES), jnp.float32),
            pltpu.VMEM((3, 2, nx, LANES), jnp.float32),
            pltpu.VMEM((KRYLOV + 1, fields, 3 * nx, ny + LANES), jnp.float32),
            pltpu.VMEM((fields, 3 * nx, ny + LANES), jnp.float32),
            pltpu.VMEM((fields, 3 * nx, ny + LANES), jnp.float32),
            pltpu.VMEM((LANES, LANES), jnp.float32),
            pltpu.VMEM((syncs, 1, LANES), jnp.float32),
            pltpu.VMEM((syncs, total, 1, LANES), jnp.float32),
            pltpu.VMEM((fields, ny), jnp.float32),
            pltpu.VMEM((n_sub * n_gx, fields, ny), jnp.float32),
            pltpu.SemaphoreType.DMA((2,)),
            pltpu.SemaphoreType.DMA((16,)),
            pltpu.SemaphoreType.DMA((16,)),
            pltpu.SemaphoreType.DMA((syncs,)),
            pltpu.SemaphoreType.DMA((syncs,)),
            pltpu.SemaphoreType.DMA((2,)),
        ],
        compiler_params=pltpu.CompilerParams(
            collective_id=0, has_side_effects=True, vmem_limit_bytes=48 * 2**20),
    )(state, damping, weights)


def solution(mesh):
    sizes = (mesh.shape["sub"], mesh.shape["gx"], mesh.shape["gy"])
    return jax.shard_map(
        functools.partial(shards, sizes),
        mesh=mesh,
        in_specs=(P(None, ("sub", "gx"), "gy"), P(None, ("sub", "gx"), "gy"), P()),
        out_specs=(P(None, ("sub", "gx"), "gy"), P(None, "gy")),
        check_vma=False,
    )
```

```python
import functools

import jax
import jax.numpy as jnp
from jax import lax
from jax.experimental import pallas as pl
from jax.experimental.pallas import tpu as pltpu
from jax.sharding import PartitionSpec as P

KRYLOV = 12
SUBSTEPS = 4
BLOCK = 4

dt_total = 4.0
sound_sq = 1.0
buoyancy_sq = 0.5
norm_eps = 1e-06
squarings = 4

SIDE = 16
LANES = 128
MESH = pl.DeviceIdType.MESH
HIGH = lax.Precision.HIGHEST


def rise(cells, axis):
    extent = cells.shape[axis]
    return 0.5 * (pltpu.roll(cells, extent - 1, axis) - pltpu.roll(cells, 1, axis))


def wave(vx, vy, b, p):
    return (
        -rise(p, 0),
        -rise(p, 1) + b,
        -buoyancy_sq * vy,
        -sound_sq * (rise(vx, 0) + rise(vy, 1)),
    )


def dot(a, b):
    return jnp.dot(a, b, precision=HIGH, preferred_element_type=jnp.float32)


def kernel(sizes, state, damping, weights_in, combined, column_error,
           weights, ext, edge_send, edge_recv, near_basis, near_stiff, basis, begin, stiff, rows_ref, send, gather,
           peak_send, peak_gather, load_sems, halo_send, halo_recv, red_send, red_recv, peak_sems):
    n_sub, n_gx, n_gy = sizes
    total = n_sub * n_gx * n_gy
    n_row = n_sub * n_gx
    fields, nx, ny = state.shape
    sub, gx, gy = lax.axis_index("sub"), lax.axis_index("gx"), lax.axis_index("gy")
    row = sub * n_gx + gx
    me = row * n_gy + gy

    def coords(flat):
        line = flat // n_gy
        return (line // n_gx, line % n_gx, flat % n_gy)

    barrier = pltpu.get_barrier_semaphore()
    loads = [
        pltpu.make_async_copy(src, ext.at[a, :, 0:nx, :], load_sems.at[a])
        for a, src in enumerate((state, damping))
    ]
    loads.append(pltpu.make_async_copy(weights_in, weights, load_sems.at[2]))
    for load in loads:
        load.start()

    subs = [lax.rem(sub + d, n_sub) for d in range(n_sub)]
    gxs = [lax.rem(gx + d, n_gx) for d in range(n_gx)]
    gys = [lax.rem(gy + d, n_gy) for d in range(n_gy)]

    def ring(d, extent):
        return min(d, extent - d)

    others = sorted(
        ((a, b, c) for a in range(n_sub) for b in range(n_gx) for c in range(n_gy)),
        key=lambda o: -(ring(o[1], n_gx) + ring(o[0], n_sub) + ring(o[2], n_gy)))[:-1]

    def each_other(visit):
        if total <= 64:
            for a, b, c in others:
                visit((subs[a], gxs[b], gys[c]))
        else:
            @pl.loop(1, total)
            def _(d):
                visit(coords((me + d) % total))

    each_other(lambda dev: pl.semaphore_signal(barrier, inc=1, device_id=dev, device_id_type=MESH))

    rows_ref[...] = jnp.zeros_like(rows_ref)
    begin[...] = jnp.zeros_like(begin)
    for load in loads:
        load.wait()

    edge = LANES // (2 * fields)
    tile_lane = lax.broadcasted_iota(jnp.int32, (nx, LANES), 1)
    for side in range(2):
        packed = jnp.zeros((nx, LANES), jnp.float32)
        for a in range(2):
            for f in range(fields):
                g = a * fields + f
                lo = 0 if side == 0 else ny - LANES
                turn = (edge * g + (0 if side == 0 else edge)) % LANES
                tile = ext[a, f, 0:nx, lo : lo + LANES]
                tile = tile if turn == 0 else pltpu.roll(tile, turn, 1)
                packed = jnp.where(tile_lane // edge == g, tile, packed)
        edge_send[side] = packed
    pl.semaphore_wait(barrier, total - 1)

    dirs = [(dr, dc) for dr in (-1, 1) for dc in (0, -1, 1)] + [(0, -1), (0, 1)]
    offset_of = {0: 0, 1: nx, -1: 2 * nx}

    def valid(dr, dc):
        r, c = row + dr, gy + dc
        return (r >= 0) & (r < n_row) & (c >= 0) & (c < n_gy)

    def landing(dr, dc):
        return edge_recv.at[dr + 1, (dc + 1) // 2]

    def halo_copies(k, deep):
        dr, dc = dirs[k]
        r = row + dr
        dev = (r // n_gx, r % n_gx, gy + dc)
        if dc == 0:
            o = offset_of[-dr]
            cut = nx - 8 if dr > 0 else 8
            lo, hi = (cut, nx) if (dr > 0) != deep else (0, cut)
            pairs = [(ext.at[a, :, lo:hi, :], ext.at[a, :, o + lo : o + hi, :]) for a in range(2)]
        else:
            pairs = [(edge_send.at[(dc + 1) // 2], landing(-dr, -dc))]
        return [
            pltpu.make_async_remote_copy(
                src_ref=src, dst_ref=dst,
                send_sem=halo_send.at[4 * k + 2 * deep + n], recv_sem=halo_recv.at[4 * k + 2 * deep + n],
                device_id=dev, device_id_type=MESH)
            for n, (src, dst) in enumerate(pairs)
        ]

    for k, (dr, dc) in enumerate(dirs):
        @pl.when(valid(dr, dc))
        def _(k=k):
            for copy in halo_copies(k, False):
                copy.start()

        @pl.when(jnp.logical_not(valid(dr, dc)))
        def _(dr=dr, dc=dc):
            if dc == 0:
                o = offset_of[dr]
                ext[:, :, o : o + nx, :] = jnp.zeros((2, fields, nx, ny), jnp.float32)
            else:
                edge_recv[dr + 1, (dc + 1) // 2] = jnp.zeros((nx, LANES), jnp.float32)

    for k, (dr, dc) in enumerate(dirs):
        if dc == 0:
            @pl.when(valid(dr, dc))
            def _(k=k):
                for copy in halo_copies(k, True):
                    copy.start()

    def arrive(deep):
        for k, (dr, dc) in enumerate(dirs):
            if dc == 0 or not deep:
                @pl.when(valid(-dr, -dc))
                def _(k=k):
                    for copy in halo_copies(k, deep):
                        copy.wait_recv()

    arrive(False)

    height, width = 3 * nx, ny + LANES
    lane = lax.broadcasted_iota(jnp.int32, (height, LANES), 1)
    sides = [
        jnp.concatenate([edge_recv[1, side], edge_recv[2, side], edge_recv[0, side]], axis=0)
        for side in range(2)
    ]

    def close(cells):
        return jnp.concatenate([cells[0 : nx + 8], cells[height - 8 : height]], axis=0)

    def extended(a, f, near):
        g = a * fields + f
        pick = close if near else lambda cells: cells

        def turned(cells, by):
            cells = pick(cells)
            return cells if by % LANES == 0 else pltpu.roll(cells, by % LANES, 1)

        left = turned(sides[0], -edge * g - edge)
        right = turned(sides[1], -edge * g)
        at = pick(lane)
        side = jnp.where(at < edge, right, jnp.where(at >= LANES - edge, left, 0.0))
        if near:
            cells = jnp.concatenate([ext[a, f, 0 : nx + 8], ext[a, f, height - 8 : height]], axis=0)
        else:
            cells = ext[a, f]
        return jnp.concatenate([cells, side], axis=1)

    rr = lax.broadcasted_iota(jnp.int32, (height, width), 0)
    cc = lax.broadcasted_iota(jnp.int32, (height, width), 1)
    has_next, has_prev = (row < n_row - 1).astype(jnp.int32), (row > 0).astype(jnp.int32)
    has_right, has_left = (gy < n_gy - 1).astype(jnp.int32), (gy > 0).astype(jnp.int32)
    row_in = jnp.where(rr < nx, 1, jnp.where(rr < 2 * nx, has_next, has_prev))
    col_in = jnp.where(cc < ny, 1, jnp.where(cc < ny + LANES // 2, has_right, has_left))
    mask = (row_in * col_in).astype(jnp.float32)

    def initial(near):
        into, rates = (near_basis, near_stiff) if near else (basis, stiff)
        valid_cells = close(mask) if near else mask
        start = [extended(0, f, near) for f in range(fields)]
        waves = wave(*start)
        for f in range(fields):
            damp = extended(1, f, near)
            s = start[f]
            rates[f] = 3.0 * damp * s * s
            into[0, f] = valid_cells * (waves[f] - damp * s * s * s)

    ri = lax.broadcasted_iota(jnp.int32, (SIDE, SIDE), 0)
    ci = lax.broadcasted_iota(jnp.int32, (SIDE, SIDE), 1)
    eye = ri == ci
    li = lax.broadcasted_iota(jnp.int32, (1, SIDE), 1)

    def to_column(r):
        return jnp.sum(jnp.where(eye, r, 0.0), axis=1, keepdims=True)

    def to_row(c):
        return jnp.sum(jnp.where(eye, c, 0.0), axis=0, keepdims=True)

    def single(x):
        return jnp.sum(jnp.sum(x, axis=1, keepdims=True), axis=0, keepdims=True)

    def combine(columns):
        return jnp.sum(columns, axis=0, keepdims=True)

    raw_gram = jnp.zeros((SIDE, SIDE), jnp.float32)
    raw_rt = jnp.zeros((SIDE, SIDE), jnp.float32)
    hess = jnp.zeros((SIDE, SIDE), jnp.float32)
    beta = None
    sent = []
    syncs = KRYLOV // BLOCK
    for s in range(syncs):
        base = s * BLOCK
        count = base + BLOCK + 1
        if s == 0:
            shift = jnp.full((1, 1), 3.0, jnp.float32)
            back = jnp.full((1, 1), 4.0, jnp.float32)
            grow = jnp.full((1, 1), 5.0, jnp.float32)
        else:
            recent = (ri >= base - 3) & (ri < base)
            third = 1.0 / 3.0
            shift = -third * single(jnp.where(recent & eye, hess, 0.0))
            back = -third * single(jnp.where(recent & (ci == ri - 1), hess, 0.0))
            grow = third * single(jnp.where(recent & (ci == ri + 1), hess, 0.0))
        inverse = 1.0 / grow

        def candidates(near, s=s, base=base, shift=shift, back=back, inverse=inverse):
            into, rates = (near_basis, near_stiff) if near else (basis, stiff)
            valid_cells = close(mask) if near else mask
            for j in range(BLOCK):
                at = base + j
                source = begin if j == 0 and s > 0 else into.at[at]
                before = begin if j == 1 and s > 0 else into.at[max(at - 1, 0)]
                current = [source[f] for f in range(fields)]
                waves = wave(*current)
                for f in range(fields):
                    image = dt_total * (valid_cells * waves[f] - rates[f] * current[f])
                    image = image + shift * current[f]
                    if j > 0:
                        image = image + back * before[f]
                    into[at + 1, f] = image * inverse

        if s == 0:
            initial(True)
        candidates(s == 0)
        vectors = near_basis if s == 0 else basis

        first = 0 if s == 0 else base + 1
        offset, offsets = 0, {}
        for j in range(first, count):
            offsets[j] = offset
            left = vectors[j, :, 0:nx, 0:ny]
            for i in range(j + 1):
                prod = left * vectors[i, :, 0:nx, 0:ny]
                prod = jnp.sum(prod, axis=0)
                prod = prod.reshape(nx // 8, 8, ny).sum(axis=0)
                acc = prod[:, 0:LANES]
                for t in range(LANES, ny, LANES):
                    acc = acc + prod[:, t : t + LANES]
                rows_ref[offset + i : offset + i + 1, :] = jnp.sum(acc, axis=0, keepdims=True)
            offset += j + 1
        packed = lax.dot_general(
            jnp.ones((8, LANES), jnp.float32), rows_ref[...], (((1,), (1,)), ((), ())),
            precision=HIGH, preferred_element_type=jnp.float32)[0:1, :]
        send[s] = packed
        gather[s, me] = packed

        each_other(lambda dev, s=s: pltpu.make_async_remote_copy(
            src_ref=send.at[s], dst_ref=gather.at[s, me],
            send_sem=red_send.at[s], recv_sem=red_recv.at[s],
            device_id=dev, device_id_type=MESH).start())

        if s == 0:
            arrive(True)
            initial(False)
            candidates(False)
        everyone = pltpu.make_async_remote_copy(
            src_ref=gather.at[s, pl.ds(0, total - 1)], dst_ref=gather.at[s, pl.ds(0, total - 1)],
            send_sem=red_send.at[s], recv_sem=red_recv.at[s],
            device_id=coords((me + 1) % total), device_id_type=MESH)
        everyone.wait_recv()
        sent.append(everyone)
        summed = jnp.sum(gather[s], axis=0)

        fresh = jnp.zeros((SIDE, LANES), jnp.float32)
        fr = lax.broadcasted_iota(jnp.int32, (SIDE, LANES), 0)
        fl = lax.broadcasted_iota(jnp.int32, (SIDE, LANES), 1)
        for j in range(first, count):
            line = summed if offsets[j] == 0 else pltpu.roll(summed, LANES - offsets[j], 1)
            fresh = jnp.where((fr == j) & (fl <= j), line, fresh)
        lower = fresh[:, 0:SIDE]
        upper = fresh.T[0:SIDE, :]
        old = (ri < first) & (ci < first)
        raw_gram = jnp.where(old, raw_gram, jnp.where(ci <= ri, lower, upper))
        if s == 0:
            gram = raw_gram
        else:
            frame = jnp.where(ri <= base, raw_rt, jnp.where(eye, 1.0, 0.0))
            gram = lax.dot_general(
                dot(frame, raw_gram), frame, (((1,), (1,)), ((), ())),
                precision=HIGH, preferred_element_type=jnp.float32)

        bt = jnp.where(ri < base, hess, 0.0)
        cand = (ri >= base) & (ri < base + BLOCK)
        bt = bt + jnp.where(cand & (ci == ri + 1), grow, 0.0) - jnp.where(cand & eye, shift, 0.0)
        bt = bt - jnp.where(cand & (ri > base) & (ci == ri - 1), back, 0.0)
        btg = dot(bt, gram)

        if s == 0:
            beta = jnp.sqrt(gram[0:1, 0:1] + norm_eps)
            known = ri < 1
            rt = jnp.where(known & eye, 1.0, 0.0) / beta
            grt = jnp.where(known, gram, 0.0) / beta
            r_col = jnp.where(ri[:, 0:1] == 0, 1.0 / beta, 0.0)
        else:
            known = ri <= base
            rt = jnp.where(known & eye, 1.0, 0.0)
            grt = jnp.where(known, gram, 0.0)
            r_col = jnp.where(ri[:, 0:1] == base, 1.0, 0.0)
        for q in range(base, base + BLOCK):
            w = combine(bt * r_col)
            u = combine(btg * r_col)
            h = jnp.sum(rt * u, axis=1, keepdims=True)
            z = w - combine(rt * h)
            gz = u - combine(grt * h)
            squared = jnp.sum(z * gz, axis=1, keepdims=True)
            z_col = to_column(z)
            length = jnp.sqrt(jnp.maximum(squared, 0.0) + norm_eps)
            scale = 1.0 / length
            r_col = z_col * scale
            rt = jnp.where(ri == q + 1, z * scale, rt)
            grt = jnp.where(ri == q + 1, gz * scale, grt)
            hess = jnp.where(ri == q, to_row(h) + jnp.where(li == q + 1, length, 0.0), hess)

        raw_rt = rt if s == 0 else dot(rt, frame)
        if s < syncs - 1:
            top = count - 1
            coefs = [raw_rt[top : top + 1, j : j + 1] for j in range(count)]
            tiles = list(range((nx + 8) // 8)) + [height // 8 - 1]
            for f in range(fields):
                for t in tiles:
                    out = None
                    for j in range(count):
                        term = coefs[j] * basis[j, f, 8 * t : 8 * t + 8, :]
                        out = term if out is None else out + term
                    begin[f, 8 * t : 8 * t + 8, :] = out

    tail = KRYLOV

    def owned(coef_row):
        out = None
        for j in range(KRYLOV + 1):
            term = coef_row[0:1, j : j + 1].reshape(1, 1, 1) * basis[j, :, 0:nx, 0:ny]
            out = term if out is None else out + term
        return out

    last = owned(raw_rt[tail : tail + 1, :])
    peak = jnp.max(jnp.abs(last), axis=1)
    peak_send[...] = peak
    peak_gather[row] = peak

    @pl.loop(1, n_row)
    def _(d):
        to = (row + d) % n_row
        pltpu.make_async_remote_copy(
            src_ref=peak_send, dst_ref=peak_gather.at[row],
            send_sem=peak_sems.at[0], recv_sem=peak_sems.at[1],
            device_id=(to // n_gx, to % n_gx, gy), device_id_type=MESH).start()

    inside = (ri < KRYLOV) & (ci < KRYLOV)
    x = jnp.where(inside, hess / SUBSTEPS, 0.0) + jnp.where((ri == KRYLOV) & (ci == 0), 1.0, 0.0)
    x = x / 2.0**squarings
    ident = jnp.where(eye, 1.0, 0.0)
    x2 = dot(x, x)
    x3 = dot(x2, x)
    x4 = dot(x2, x2)
    fact = [1.0]
    for d in range(1, 13):
        fact.append(fact[-1] / d)

    def poly(d):
        return fact[d] * ident + fact[d + 1] * x + fact[d + 2] * x2 + fact[d + 3] * x3

    power = poly(0) + dot(x4, poly(4) + dot(x4, poly(8) + fact[12] * x4))
    for repeat in range(squarings):
        power = dot(power, power)
    powers = [None, power]
    for member in range(2, SUBSTEPS + 1):
        powers.append(dot(powers[member // 2], powers[member - member // 2]))
    mixing = jnp.zeros((1, SIDE), jnp.float32)
    highest = jnp.zeros((1, 1), jnp.float32)
    tip = hess[KRYLOV - 1 : KRYLOV, KRYLOV : KRYLOV + 1]
    for member in range(SUBSTEPS):
        line = powers[member + 1][KRYLOV : KRYLOV + 1, :]
        part = (dt_total / SUBSTEPS) * beta * line
        mixing = mixing + weights[member] * part
        fraction = (member + 1) / SUBSTEPS
        highest = jnp.maximum(highest, fraction * tip * jnp.abs(part[:, KRYLOV - 1 : KRYLOV]))
    mixing = jnp.where(li < KRYLOV, mixing, 0.0)
    combined[...] = ext[0, :, 0:nx, :] + owned(combine(raw_rt * to_column(mixing)))

    around = pltpu.make_async_remote_copy(
        src_ref=peak_gather.at[pl.ds(0, n_row - 1)], dst_ref=peak_gather.at[pl.ds(0, n_row - 1)],
        send_sem=peak_sems.at[0], recv_sem=peak_sems.at[1],
        device_id=coords((me + n_gy) % total), device_id_type=MESH)
    around.wait_recv()
    for copy in sent + [around]:
        copy.wait_send()
    for k, (dr, dc) in enumerate(dirs):
        @pl.when(valid(dr, dc))
        def _(k=k, dc=dc):
            for copy in halo_copies(k, False) + (halo_copies(k, True) if dc == 0 else []):
                copy.wait_send()

    column_error[...] = highest * jnp.max(peak_gather[...], axis=0)


def shards(sizes, state, damping, weights):
    fields, nx, ny = state.shape
    n_sub, n_gx, n_gy = sizes
    total = n_sub * n_gx * n_gy
    syncs = KRYLOV // BLOCK
    vmem = pl.BlockSpec(memory_space=pltpu.VMEM)
    return pl.pallas_call(
        functools.partial(kernel, sizes),
        out_shape=(
            jax.ShapeDtypeStruct(state.shape, jnp.float32),
            jax.ShapeDtypeStruct((fields, ny), jnp.float32),
        ),
        in_specs=[pl.BlockSpec(memory_space=pltpu.HBM)] * 3,
        out_specs=(vmem, vmem),
        scratch_shapes=[
            pltpu.SMEM(weights.shape, jnp.float32),
            pltpu.VMEM((2, fields, 3 * nx, ny), jnp.float32),
            pltpu.VMEM((2, nx, LANES), jnp.float32),
            pltpu.VMEM((3, 2, nx, LANES), jnp.float32),
            pltpu.VMEM((BLOCK + 1, fields, nx + 16, ny + LANES), jnp.float32),
            pltpu.VMEM((fields, nx + 16, ny + LANES), jnp.float32),
            pltpu.VMEM((KRYLOV + 1, fields, 3 * nx, ny + LANES), jnp.float32),
            pltpu.VMEM((fields, 3 * nx, ny + LANES), jnp.float32),
            pltpu.VMEM((fields, 3 * nx, ny + LANES), jnp.float32),
            pltpu.VMEM((LANES, LANES), jnp.float32),
            pltpu.VMEM((syncs, 1, LANES), jnp.float32),
            pltpu.VMEM((syncs, total, 1, LANES), jnp.float32),
            pltpu.VMEM((fields, ny), jnp.float32),
            pltpu.VMEM((n_sub * n_gx, fields, ny), jnp.float32),
            pltpu.SemaphoreType.DMA((3,)),
            pltpu.SemaphoreType.DMA((32,)),
            pltpu.SemaphoreType.DMA((32,)),
            pltpu.SemaphoreType.DMA((syncs,)),
            pltpu.SemaphoreType.DMA((syncs,)),
            pltpu.SemaphoreType.DMA((2,)),
        ],
        compiler_params=pltpu.CompilerParams(
            collective_id=0, has_side_effects=True, vmem_limit_bytes=67043328),
    )(state, damping, weights)


def solution(mesh):
    sizes = (mesh.shape["sub"], mesh.shape["gx"], mesh.shape["gy"])
    return jax.shard_map(
        functools.partial(shards, sizes),
        mesh=mesh,
        in_specs=(P(None, ("sub", "gx"), "gy"), P(None, ("sub", "gx"), "gy"), P()),
        out_specs=(P(None, ("sub", "gx"), "gy"), P(None, "gy")),
        check_vma=False,
    )
```
